32 devices in a mesh: section: 4 (over x, core), tensor: 8 (over z, y).
Axes of the slice: x: 2, y: 2, z: 4, core: 2. Of those that a mesh axis runs over, the one named last changes fastest.
Arguments:
- hidden_in: bfloat16 [64, 2560], P(None, 'tensor'), may hold values from -6 to 6
- pre_gain: float32 [4, 2560], P('section'), may hold values from 0.1 to 1.9
- w_zx: bfloat16 [4, 2560, 80, 128], P('section', None, 'tensor'), may hold values from -0.125 to 0.125
- w_bc: bfloat16 [4, 2560, 256], P('section'), may hold values from -0.125 to 0.125
- w_dt: bfloat16 [4, 2560, 80], P('section', None, 'tensor'), may hold values from -0.125 to 0.125
- dt_bias: float32 [4, 80], P('section', 'tensor'), may hold values from -4 to -1
- a_log: float32 [4, 80], P('section', 'tensor'), may hold values from 0 to 2.77
- d_skip: float32 [4, 80], P('section', 'tensor'), may hold values from 0.5 to 2
- conv_x_weight: float32 [4, 4, 80, 64], P('section', None, 'tensor'), may hold values from -3 to 3
- conv_x_bias: float32 [4, 80, 64], P('section', 'tensor'), may hold values from -3 to 3
- conv_bc_weight: float32 [4, 4, 256], P('section'), may hold values from -3 to 3
- conv_bc_bias: float32 [4, 256], P('section'), may hold values from -3 to 3
- inner_gain: float32 [4, 80, 64], P('section', 'tensor'), may hold values from 0.1 to 1.9
- w_out: bfloat16 [4, 80, 64, 2560], P('section', 'tensor'), may hold values from -0.078125 to 0.078125
- conv_x_state: bfloat16 [4, 64, 3, 80, 64], P('section', None, None, 'tensor'), may hold values from -6 to 6
- conv_bc_state: bfloat16 [4, 64, 3, 256], P('section'), may hold values from -6 to 6
- ssm_state: bfloat16 [4, 64, 80, 64, 128], P('section', None, 'tensor'), may hold values from -14 to 14
Outputs:
- section_hidden: bfloat16 [4, 64, 2560], P('section', None, 'tensor')
- conv_x_new: bfloat16 [4, 64, 3, 80, 64], P('section', None, None, 'tensor')
- conv_bc_new: bfloat16 [4, 64, 3, 256], P('section')
- ssm_new: bfloat16 [4, 64, 80, 64, 128], P('section', None, 'tensor')
The draws below stay inside these ranges and needn't reach their ends.
All inputs are finite; a program needn't handle non-finite values.
Results may differ from the reference program's by a relative error of at most 0.02.
Values may be sent and summed in bfloat16 or wider, within the bound.
No kernel may reach another device: no remote copies, remote signals or barrier semaphores. Data moves between devices by JAX's collectives and lax.ppermute only.
A program may use at most 128 MiB of HBM per device.

```python
import jax
import jax.numpy as jnp
from jax import lax

D = 2560
H = 80
P_SIZE = 64
N = 128
K = 4
L_DEV = 1
STREAMS = 64
LAYERS = 4


def draw_ssm_state(key, part):
    heads = jnp.arange(H, dtype=jnp.float32) / (H - 1)
    scales = 0.5 * 8.0 ** heads
    values = jnp.clip(jax.random.normal(key, (LAYERS, STREAMS, H, P_SIZE, N), jnp.float32), -3.5, 3.5)
    return (values * scales[None, None, :, None, None]).astype(jnp.bfloat16)


def block_scale(rng, extent, pieces, smallest, largest):
    level = 1.0
    for axis_at, parts in pieces:
        draws = jax.random.uniform(jax.random.fold_in(jax.random.fold_in(rng, 6), axis_at), (parts,), jnp.float32, smallest / len(pieces), largest / len(pieces))
        level = level * jnp.repeat(jnp.exp(draws), extent[axis_at] // parts).reshape((-1,) + (1,) * (len(extent) - 1 - axis_at))
    return level


def centred(own_key, shape, scale, bound, cuts=(), kind=jnp.bfloat16):
    values = jax.random.normal(own_key, shape, jnp.float32) * scale
    if len(cuts) > 0:
        values = block_scale(own_key, shape, cuts, -0.22, 0.18) * values
    return jnp.clip(values, min=-bound, max=bound).astype(kind)


def setup_inputs(seed: int = 0) -> dict:
    key_of = jax.random.split(jax.random.key(seed), 18)
    hidden_in = centred(key_of[0], (STREAMS, D), 1.0, 6.0, ((1, 8),))
    pre_gain = jnp.clip(1.0 + 0.18 * jax.random.normal(key_of[1], (LAYERS, D), jnp.float32), 0.1, 1.9)
    w_zx = centred(key_of[2], (LAYERS, D, H, 2 * P_SIZE), D ** -0.5, 0.125, ((0, 4), (2, 8)))
    w_bc = centred(key_of[3], (LAYERS, D, 2 * N), D ** -0.5, 0.125, ((0, 4),))
    w_dt = centred(key_of[4], (LAYERS, D, H), D ** -0.5, 0.125, ((0, 4), (2, 8)))
    dt_bias = jnp.clip(-4.0 + 3.0 * jax.random.uniform(key_of[5], (LAYERS, H), jnp.float32) ** block_scale(key_of[5], (LAYERS, H), ((0, 4), (1, 8)), -0.2, 0.2), -4.0, -1.0)
    a_log = jnp.clip(2.77 * jax.random.uniform(key_of[6], (LAYERS, H), jnp.float32) ** block_scale(key_of[6], (LAYERS, H), ((0, 4), (1, 8)), -0.2, 0.2), 0.0, 2.77)
    d_skip = jnp.clip(0.5 + 1.5 * jax.random.uniform(key_of[7], (LAYERS, H), jnp.float32) ** block_scale(key_of[7], (LAYERS, H), ((0, 4), (1, 8)), -0.2, 0.2), 0.5, 2.0)
    conv_x_weight = centred(key_of[8], (LAYERS, K, H, P_SIZE), K ** -0.5, 3.0, ((0, 4), (2, 8)), jnp.float32)
    conv_x_bias = centred(key_of[9], (LAYERS, H, P_SIZE), 0.5, 3.0, ((0, 4), (1, 8)), jnp.float32)
    conv_bc_weight = centred(key_of[10], (LAYERS, K, 2 * N), K ** -0.5, 3.0, ((0, 4),), jnp.float32)
    conv_bc_bias = centred(key_of[11], (LAYERS, 2 * N), 0.5, 3.0, ((0, 4),), jnp.float32)
    inner_gain = jnp.clip(1.0 + 0.18 * jax.random.normal(key_of[12], (LAYERS, H, P_SIZE), jnp.float32), 0.1, 1.9)
    w_out = centred(key_of[13], (LAYERS, H, P_SIZE, D), (H * P_SIZE) ** -0.5, 0.078125, ((0, 4), (1, 8)))
    conv_x_state = centred(key_of[14], (LAYERS, STREAMS, K - 1, H, P_SIZE), 1.0, 6.0, ((0, 4), (3, 8)))
    conv_bc_state = centred(key_of[15], (LAYERS, STREAMS, K - 1, 2 * N), 1.0, 6.0, ((0, 4),))
    ssm_state = draw_ssm_state(jax.random.fold_in(key_of[17], 71), 0)
    return {"hidden_in": hidden_in, "pre_gain": pre_gain, "w_zx": w_zx, "w_bc": w_bc, "w_dt": w_dt, "dt_bias": dt_bias, "a_log": a_log, "d_skip": d_skip, "conv_x_weight": conv_x_weight, "conv_x_bias": conv_x_bias, "conv_bc_weight": conv_bc_weight, "conv_bc_bias": conv_bc_bias, "inner_gain": inner_gain, "w_out": w_out, "conv_x_state": conv_x_state, "conv_bc_state": conv_bc_state, "ssm_state": ssm_state}


epsilon = 1e-05

def mixer_core(normed, w_zx, w_bc, w_dt, dt_bias, a_log, d_skip, conv_x_weight, conv_x_bias, conv_bc_weight, conv_bc_bias, conv_x_state, conv_bc_state, ssm_state):
    row_count = normed.shape[0]
    model_width = w_zx.shape[0]
    head_count = w_zx.shape[1]
    head_size = w_zx.shape[2] // 2
    state_size = w_bc.shape[1] // 2
    both_parts = jnp.dot(normed, w_zx.reshape(model_width, head_count * 2 * head_size), preferred_element_type=jnp.float32)
    both_parts = both_parts.reshape(row_count, head_count, 2 * head_size)
    gate_z = both_parts[:, :, :head_size]
    x_fresh = both_parts[:, :, head_size:].astype(jnp.bfloat16)
    bc_fresh = jnp.dot(normed, w_bc, preferred_element_type=jnp.float32).astype(jnp.bfloat16)
    dt_raw = jnp.dot(normed, w_dt, preferred_element_type=jnp.float32)
    x_window = jnp.concatenate([conv_x_state, x_fresh[:, None]], axis=1)
    bc_window = jnp.concatenate([conv_bc_state, bc_fresh[:, None]], axis=1)
    x_conv = jax.nn.silu(lax.optimization_barrier(jnp.sum(x_window.astype(jnp.float32) * conv_x_weight[None], axis=1)) + conv_x_bias[None])
    bc_conv = jax.nn.silu(lax.optimization_barrier(jnp.sum(bc_window.astype(jnp.float32) * conv_bc_weight[None], axis=1)) + conv_bc_bias[None])
    b_input = bc_conv[:, :state_size]
    c_output = bc_conv[:, state_size:]
    step_size = jax.nn.softplus(dt_raw + dt_bias[None])
    decay_rate = jnp.exp(-step_size * jnp.exp(a_log)[None])
    state_f = decay_rate[:, :, None, None] * ssm_state.astype(jnp.float32) + (step_size[:, :, None] * x_conv)[:, :, :, None] * b_input[:, None, None, :]
    y_out = lax.optimization_barrier(jnp.sum(state_f * c_output[:, None, None, :], axis=-1)) + d_skip[None, :, None] * x_conv
    gated_out = y_out * jax.nn.silu(gate_z)
    return (gated_out, x_window[:, 1:], bc_window[:, 1:], state_f.astype(jnp.bfloat16))

def reference(hidden_in, pre_gain, w_zx, w_bc, w_dt, dt_bias, a_log, d_skip, conv_x_weight, conv_x_bias, conv_bc_weight, conv_bc_bias, inner_gain, w_out, conv_x_state, conv_bc_state, ssm_state):
    hidden = hidden_in
    section_list = []
    conv_x_list = []
    conv_bc_list = []
    ssm_list = []
    for which_layer in range(LAYERS):
        wide = hidden.astype(jnp.float32)
        normed = (wide * lax.rsqrt(lax.optimization_barrier(jnp.mean(wide * wide, axis=-1, keepdims=True)) + epsilon) * pre_gain[which_layer][None]).astype(jnp.bfloat16)
        gated_out, conv_x_next, conv_bc_next, ssm_next = mixer_core(normed, w_zx[which_layer], w_bc[which_layer], w_dt[which_layer], dt_bias[which_layer], a_log[which_layer], d_skip[which_layer], conv_x_weight[which_layer], conv_x_bias[which_layer], conv_bc_weight[which_layer], conv_bc_bias[which_layer], conv_x_state[which_layer], conv_bc_state[which_layer], ssm_state[which_layer])
        squares = lax.optimization_barrier(jnp.mean(gated_out * gated_out, axis=(1, 2)))
        scaled_inner = (gated_out * inner_gain[which_layer][None]).astype(jnp.bfloat16)
        head_count = scaled_inner.shape[1]
        head_size = scaled_inner.shape[2]
        product = jnp.dot(scaled_inner.reshape(scaled_inner.shape[0], head_count * head_size), w_out[which_layer].reshape(head_count * head_size, w_out.shape[-1]), preferred_element_type=jnp.float32)
        mixed = product * lax.rsqrt(squares + epsilon)[:, None]
        hidden = (wide + mixed).astype(jnp.bfloat16)
        conv_x_list.append(conv_x_next)
        conv_bc_list.append(conv_bc_next)
        ssm_list.append(ssm_next)
        if (which_layer + 1) % L_DEV == 0:
            section_list.append(hidden)
    return (jnp.stack(section_list), jnp.stack(conv_x_list), jnp.stack(conv_bc_list), jnp.stack(ssm_list))
```

```python
import jax
import jax.numpy as jnp
from jax import lax
from jax.sharding import PartitionSpec as P

epsilon = 1e-05


def gather_shares(share):
    count = lax.axis_size("tensor")
    spread = jnp.broadcast_to(share[None], (count,) + share.shape)
    return lax.all_to_all(spread, "tensor", 0, 0, tiled=True)


def shards(
    hidden_in,
    pre_gain,
    w_zx,
    w_bc,
    w_dt,
    dt_bias,
    a_log,
    d_skip,
    conv_x_weight,
    conv_x_bias,
    conv_bc_weight,
    conv_bc_bias,
    inner_gain,
    w_out,
    conv_x_state,
    conv_bc_state,
    ssm_state,
):
    section_count = lax.axis_size("section")
    tensor_count = lax.axis_size("tensor")
    section_at = lax.axis_index("section")
    streams, share_cols = hidden_in.shape
    width = w_zx.shape[1]
    heads = w_zx.shape[2]
    head_size = w_zx.shape[3] // 2
    state_size = w_bc.shape[2] // 2
    inner = heads * head_size
    all_channels = inner * tensor_count
    w_heads = jnp.transpose(w_zx[0], (1, 0, 2))
    state = ssm_state[0]

    def live(share, saved):
        shares = gather_shares(share)
        full = jnp.transpose(shares, (1, 0, 2)).reshape(streams, width)
        wide = full.astype(jnp.float32)
        normed = (
            wide
            * lax.rsqrt(jnp.mean(wide * wide, axis=-1, keepdims=True) + epsilon)
            * pre_gain[0][None]
        ).astype(jnp.bfloat16)
        zx = jnp.einsum("sd,hdc->shc", normed, w_heads, preferred_element_type=jnp.float32)
        gate_z = zx[:, :, :head_size]
        x_fresh = zx[:, :, head_size:].astype(jnp.bfloat16)
        bc_fresh = jnp.dot(normed, w_bc[0], preferred_element_type=jnp.float32).astype(jnp.bfloat16)
        dt_raw = jnp.dot(normed, w_dt[0], preferred_element_type=jnp.float32)
        x_window = jnp.concatenate([conv_x_state[0], x_fresh[:, None]], axis=1)
        bc_window = jnp.concatenate([conv_bc_state[0], bc_fresh[:, None]], axis=1)
        x_conv = jax.nn.silu(
            jnp.sum(x_window.astype(jnp.float32) * conv_x_weight[0][None], axis=1)
            + conv_x_bias[0][None]
        )
        bc_conv = jax.nn.silu(
            jnp.sum(bc_window.astype(jnp.float32) * conv_bc_weight[0][None], axis=1)
            + conv_bc_bias[0][None]
        )
        b_input = bc_conv[:, :state_size]
        c_output = bc_conv[:, state_size:]
        step_size = jax.nn.softplus(dt_raw + dt_bias[0][None])
        decay = jnp.exp(-step_size * jnp.exp(a_log[0])[None])
        stepped = step_size[:, :, None] * x_conv
        old_part = jnp.sum(state.astype(jnp.float32) * c_output[:, None, None, :], axis=-1)
        overlap = jnp.sum(b_input * c_output, axis=-1)
        y_out = (
            decay[:, :, None] * old_part
            + stepped * overlap[:, None, None]
            + d_skip[0][None, :, None] * x_conv
        )
        gated = y_out * jax.nn.silu(gate_z)
        squares = jnp.sum(gated * gated, axis=(1, 2))
        scaled = (gated * inner_gain[0][None]).astype(jnp.bfloat16)
        partial = jnp.dot(
            scaled.reshape(streams, inner),
            w_out[0].reshape(inner, width),
            preferred_element_type=jnp.float32,
        )
        pieces = partial.astype(jnp.bfloat16).reshape(streams, tensor_count, share_cols)
        pieces = jnp.transpose(pieces, (1, 0, 2))
        high = squares.astype(jnp.bfloat16)
        low = (squares - high.astype(jnp.float32)).astype(jnp.bfloat16)
        tail = jnp.stack([high, low], axis=1)[None]
        tail = jnp.broadcast_to(tail, (tensor_count, streams, 2))
        sent = jnp.concatenate([pieces, tail], axis=2)
        got = lax.all_to_all(sent, "tensor", 0, 0, tiled=True).astype(jnp.float32)
        total = jnp.sum(got, axis=0)
        squares_all = total[:, share_cols] + total[:, share_cols + 1]
        factor = lax.rsqrt(squares_all / all_channels + epsilon)[:, None]
        fresh = (share.astype(jnp.float32) + total[:, :share_cols] * factor).astype(jnp.bfloat16)
        return fresh, (x_fresh, bc_fresh, stepped, b_input, decay)

    saved = (
        jnp.zeros((streams, heads, head_size), jnp.bfloat16),
        jnp.zeros((streams, 2 * state_size), jnp.bfloat16),
        jnp.zeros((streams, heads, head_size), jnp.float32),
        jnp.zeros((streams, state_size), jnp.float32),
        jnp.zeros((streams, heads), jnp.float32),
    )
    incoming = hidden_in
    section_share = jnp.zeros_like(hidden_in)
    for tick in range(section_count):
        is_live = section_at == tick
        section_share, saved = lax.cond(
            is_live,
            lambda share, kept, old: live(share, old),
            lambda share, kept, old: (kept, old),
            incoming,
            section_share,
            saved,
        )
        if tick + 1 < section_count:
            ring = [(at, (at + 1) % section_count) for at in range(section_count)]
            incoming = lax.ppermute(section_share, "section", ring)
    x_fresh, bc_fresh, stepped, b_input, decay = saved
    state_f = (
        decay[:, :, None, None] * state.astype(jnp.float32)
        + stepped[:, :, :, None] * b_input[:, None, None, :]
    )
    conv_x_new = jnp.concatenate([conv_x_state[0][:, 1:], x_fresh[:, None]], axis=1)
    conv_bc_new = jnp.concatenate([conv_bc_state[0][:, 1:], bc_fresh[:, None]], axis=1)
    return (
        section_share[None],
        conv_x_new[None],
        conv_bc_new[None],
        state_f.astype(jnp.bfloat16)[None],
    )


def solution(mesh):
    placed = (
        P(None, "tensor"),
        P("section", None),
        P("section", None, "tensor", None),
        P("section", None, None),
        P("section", None, "tensor"),
        P("section", "tensor"),
        P("section", "tensor"),
        P("section", "tensor"),
        P("section", None, "tensor", None),
        P("section", "tensor", None),
        P("section", None, None),
        P("section", None),
        P("section", "tensor", None),
        P("section", "tensor", None, None),
        P("section", None, None, "tensor", None),
        P("section", None, None, None),
        P("section", None, "tensor", None, None),
    )
    return jax.shard_map(
        shards,
        mesh=mesh,
        in_specs=placed,
        out_specs=(
            P("section", None, "tensor"),
            P("section", None, None, "tensor", None),
            P("section", None, None, None),
            P("section", None, "tensor", None, None),
        ),
        check_vma=False,
    )
```

```python
import functools

import jax
import jax.numpy as jnp
from jax import lax
from jax.experimental import pallas as pl
from jax.experimental.pallas import tpu as pltpu
from jax.sharding import PartitionSpec as P

epsilon = 1e-05
row_block = 8
wide_lanes = 128
input_count = 16
in_flight = 3


def silu(value):
    return value / (1.0 + jnp.exp(-value))


def split_two(value):
    high = value.astype(jnp.bfloat16)
    low = (value - high.astype(jnp.float32)).astype(jnp.bfloat16)
    return high, low


def layer_math(
    shares,
    gain,
    w_heads,
    w_bc,
    w_dt,
    dt_bias,
    a_log,
    d_skip,
    conv_x_weight,
    conv_x_bias,
    conv_bc_weight,
    conv_bc_bias,
    inner_gain,
    w_out,
    conv_x_state,
    conv_bc_state,
    state,
    wait_heads,
    wait_out,
    wait_state,
    sent,
    conv_x_out,
    conv_bc_out,
    stepped_out,
    decay_out,
    b_out,
    old_part,
    gated_buf,
):
    parts, streams, share_cols = shares.shape
    heads, width, lanes = w_heads.shape
    head_size = lanes // 2
    state_size = w_bc.shape[1] // 2
    inner = heads * head_size
    blocks = streams // row_block

    wide = [shares[at].astype(jnp.float32) for at in range(parts)]
    square = sum(jnp.sum(piece * piece, axis=-1, keepdims=True) for piece in wide)
    scale = lax.rsqrt(square / width + epsilon)
    normed = jnp.concatenate(wide, axis=1) * scale * gain[...]
    normed = normed.astype(jnp.bfloat16)

    bc_fresh = jnp.dot(normed, w_bc[...], preferred_element_type=jnp.float32).astype(jnp.bfloat16)
    taps = conv_bc_weight[...]
    count = taps.shape[0]
    for tap in range(count - 2):
        conv_bc_out[tap] = conv_bc_state[tap + 1]
        conv_x_out[tap] = conv_x_state[tap + 1]
    conv_bc_out[count - 2] = bc_fresh
    bc_sum = bc_fresh.astype(jnp.float32) * taps[count - 1 : count]
    for tap in range(count - 1):
        bc_sum = bc_sum + conv_bc_state[tap].astype(jnp.float32) * taps[tap : tap + 1]
    bc_conv = silu(bc_sum + conv_bc_bias[...])
    b_input = bc_conv[:, :state_size]
    c_output = bc_conv[:, state_size:]
    b_out[...] = b_input
    overlap = jnp.sum(b_input * c_output, axis=-1, keepdims=True)
    dt_raw = lax.dot_general(
        normed, w_dt[...], (((1,), (1,)), ((), ())), preferred_element_type=jnp.float32
    )
    step_size = jax.nn.softplus(dt_raw + dt_bias[...])
    decay = jnp.exp(-step_size * jnp.exp(a_log[...]))
    decay_out[...] = decay

    c_high, c_low = split_two(c_output)
    row_at = lax.broadcasted_iota(jnp.int32, (row_block, inner), 0)
    for block in range(blocks):
        wait_state(block)
        first = block * row_block
        both = jnp.concatenate(
            [
                c_high[first : first + row_block].astype(jnp.float32),
                c_low[first : first + row_block].astype(jnp.float32),
            ],
            axis=0,
        ).astype(jnp.bfloat16)
        kept = jnp.zeros((row_block, inner), jnp.float32)
        for row in range(row_block):
            product = lax.dot_general(
                both,
                state[first + row],
                (((1,), (1,)), ((), ())),
                preferred_element_type=jnp.float32,
            )
            kept = jnp.where(row_at == row, product[:row_block] + product[row_block:], kept)
        old_part[first : first + row_block, :] = kept

    squares = jnp.zeros((streams, 1), jnp.float32)
    for head in range(heads):
        wait_heads(head)
        zx = jnp.dot(normed, w_heads[head], preferred_element_type=jnp.float32)
        gate = zx[:, :head_size]
        x_fresh = zx[:, head_size:].astype(jnp.bfloat16)
        conv_x_out[count - 2, head] = x_fresh
        taps = conv_x_weight[head]
        x_sum = x_fresh.astype(jnp.float32) * taps[count - 1 : count]
        for tap in range(count - 1):
            x_sum = x_sum + conv_x_state[tap, head].astype(jnp.float32) * taps[tap : tap + 1]
        x_conv = silu(x_sum + conv_x_bias[head])
        stepped = x_conv * step_size[:, head : head + 1]
        span = slice(head * head_size, (head + 1) * head_size)
        stepped_out[:, span] = stepped
        faded = decay[:, head : head + 1]
        y_out = faded * old_part[:, span] + stepped * overlap + d_skip[:, head : head + 1] * x_conv
        gated = y_out * silu(gate)
        squares = squares + jnp.sum(gated * gated, axis=-1, keepdims=True)
        gated_buf[:, span] = gated * inner_gain[head]

    scaled = gated_buf[...].astype(jnp.bfloat16)
    wait_out()
    partial = jnp.dot(scaled, w_out[...], preferred_element_type=jnp.float32)
    tail_cols = sent.shape[2] - share_cols
    high, low = split_two(squares)
    lane_at = lax.broadcasted_iota(jnp.int32, (streams, tail_cols), 1)
    tail = jnp.where(
        lane_at == 0,
        high.astype(jnp.float32),
        jnp.where(lane_at == 1, low.astype(jnp.float32), 0.0),
    )
    for at in range(parts):
        piece = partial[:, at * share_cols : (at + 1) * share_cols]
        sent[at] = jnp.concatenate([piece, tail], axis=1).astype(jnp.bfloat16)


def layer_body(shares, *refs):
    inputs = refs[:input_count]
    outputs = refs[input_count : input_count + 6]
    buffers = refs[input_count + 6 : 2 * input_count + 6]
    small_sem, heads_sem, out_sem, state_sem, old_part, gated_buf = refs[2 * input_count + 6 :]
    heads = inputs[1].shape[0]
    blocks = inputs[-1].shape[0] // row_block
    large = (1, 12, input_count - 1)

    def rows(block):
        return pl.ds(block * row_block, row_block)

    small_copies = [
        pltpu.make_async_copy(inputs[at], buffers[at], small_sem.at[at])
        for at in range(input_count)
        if at not in large
    ]
    state_copies = [
        pltpu.make_async_copy(inputs[-1].at[rows(at)], buffers[-1].at[rows(at)], state_sem.at[at])
        for at in range(blocks)
    ]
    head_copies = [
        pltpu.make_async_copy(inputs[1].at[at], buffers[1].at[at], heads_sem.at[at])
        for at in range(heads)
    ]
    out_copy = pltpu.make_async_copy(inputs[12], buffers[12], out_sem)
    for copy in small_copies:
        copy.start()
    ordered = state_copies + head_copies + [out_copy]
    for copy in ordered[:in_flight]:
        copy.start()
    for copy in small_copies:
        copy.wait()

    def arrive(at):
        ordered[at].wait()
        if at + in_flight < len(ordered):
            ordered[at + in_flight].start()

    layer_math(
        shares,
        *buffers,
        lambda head: arrive(blocks + head),
        lambda: arrive(blocks + heads),
        arrive,
        *outputs,
        old_part,
        gated_buf,
    )


def update_body(old, stepped, decay, b_input, out, state, fresh_buf, in_sems, sems):
    streams, inner, size = state.shape
    heads = decay.shape[1]
    head_size = inner // heads
    blocks = streams // row_block

    def enter(block):
        rows = pl.ds(block * row_block, row_block)
        return pltpu.make_async_copy(old.at[rows], state.at[rows], in_sems.at[block])

    def leave(block):
        rows = pl.ds(block * row_block, row_block)
        return pltpu.make_async_copy(fresh_buf.at[rows], out.at[rows], sems.at[block])

    def step(block, carry):
        first = pl.multiple_of(block * row_block, row_block)
        enter(block).wait()

        @pl.when(block + in_flight < blocks)
        def _():
            enter(block + in_flight).start()

        stepped_t = jnp.transpose(stepped[pl.ds(first, row_block), :])
        faded_rows = decay[pl.ds(first, row_block), :]
        b_rows = b_input[pl.ds(first, row_block), :]
        for row in range(row_block):
            b_row = jnp.broadcast_to(b_rows[row : row + 1], (head_size, size))
            for head in range(heads):
                span = slice(head * head_size, (head + 1) * head_size)
                column = jnp.broadcast_to(stepped_t[span, row : row + 1], (head_size, size))
                faded = jnp.broadcast_to(faded_rows[row : row + 1, head : head + 1], (head_size, size))
                fresh = faded * state[first + row, span].astype(jnp.float32) + column * b_row
                fresh_buf[first + row, span] = fresh.astype(jnp.bfloat16)
        leave(block).start()
        return carry

    for block in range(min(in_flight, blocks)):
        enter(block).start()
    lax.fori_loop(0, blocks, step, 0)
    for block in range(blocks):
        leave(block).wait()


def whole(memory=pltpu.VMEM):
    return pl.BlockSpec(memory_space=memory)


def run_layer(*operands):
    shares, gain, w_heads, w_bc, w_dt = operands[:5]
    w_out, conv_x_state, conv_bc_state, state = operands[13:]
    parts, streams, share_cols = shares.shape
    heads, width, lanes = w_heads.shape
    head_size = lanes // 2
    inner = heads * head_size
    both = w_bc.shape[1]
    sent_cols = -(-(share_cols + 2) // wide_lanes) * wide_lanes
    flops = 2 * streams * (width * (heads * lanes + both + inner)) + 2 * state.size
    moved = 2 * (w_heads.size + w_bc.size + w_out.size + state.size)
    return pl.pallas_call(
        layer_body,
        in_specs=[whole()] + [whole(pltpu.HBM) for _ in operands[1:]],
        out_specs=tuple(whole() for _ in range(6)),
        out_shape=(
            jax.ShapeDtypeStruct((parts, streams, sent_cols), jnp.bfloat16),
            jax.ShapeDtypeStruct(conv_x_state.shape, jnp.bfloat16),
            jax.ShapeDtypeStruct(conv_bc_state.shape, jnp.bfloat16),
            jax.ShapeDtypeStruct((streams, inner), jnp.float32),
            jax.ShapeDtypeStruct((streams, heads), jnp.float32),
            jax.ShapeDtypeStruct((streams, both // 2), jnp.float32),
        ),
        scratch_shapes=[pltpu.VMEM(operand.shape, operand.dtype) for operand in operands[1:]]
        + [
            pltpu.SemaphoreType.DMA((input_count,)),
            pltpu.SemaphoreType.DMA((heads,)),
            pltpu.SemaphoreType.DMA(()),
            pltpu.SemaphoreType.DMA((streams // row_block,)),
            pltpu.VMEM((streams, inner), jnp.float32),
            pltpu.VMEM((streams, inner), jnp.float32),
        ],
        compiler_params=pltpu.CompilerParams(vmem_limit_bytes=44 * 1024 * 1024),
        cost_estimate=pl.CostEstimate(flops=flops, transcendentals=0, bytes_accessed=moved),
        name="layer",
    )(*operands)


def run_update(state, stepped, decay, b_input):
    blocks = state.shape[0] // row_block
    return pl.pallas_call(
        update_body,
        in_specs=[whole(pltpu.HBM)] + [whole() for _ in range(3)],
        out_specs=whole(pltpu.HBM),
        out_shape=jax.ShapeDtypeStruct(state.shape, state.dtype),
        scratch_shapes=[
            pltpu.VMEM(state.shape, state.dtype),
            pltpu.VMEM(state.shape, state.dtype),
            pltpu.SemaphoreType.DMA((blocks,)),
            pltpu.SemaphoreType.DMA((blocks,)),
        ],
        compiler_params=pltpu.CompilerParams(vmem_limit_bytes=24 * 1024 * 1024),
        cost_estimate=pl.CostEstimate(
            flops=40 * state.size, transcendentals=0, bytes_accessed=4 * state.size
        ),
        name="update",
    )(state, stepped, decay, b_input)


def gather_shares(share):
    count = lax.axis_size("tensor")
    spread = jnp.broadcast_to(share[None], (count,) + share.shape)
    return lax.all_to_all(spread, "tensor", 0, 0, tiled=True)


def shards(
    hidden_in,
    pre_gain,
    w_zx,
    w_bc,
    w_dt,
    dt_bias,
    a_log,
    d_skip,
    conv_x_weight,
    conv_x_bias,
    conv_bc_weight,
    conv_bc_bias,
    inner_gain,
    w_out,
    conv_x_state,
    conv_bc_state,
    ssm_state,
):
    section_count = lax.axis_size("section")
    tensor_count = lax.axis_size("tensor")
    section_at = lax.axis_index("section")
    streams, share_cols = hidden_in.shape
    width = w_zx.shape[1]
    heads = w_zx.shape[2]
    head_size = w_zx.shape[3] // 2
    both = w_bc.shape[2]
    inner = heads * head_size
    all_channels = inner * tensor_count
    state = ssm_state[0].reshape(streams, inner, both // 2)
    x_old = jnp.transpose(conv_x_state[0], (1, 2, 0, 3))
    bc_old = jnp.transpose(conv_bc_state[0], (1, 0, 2))
    layer_args = (
        pre_gain,
        jnp.transpose(w_zx[0], (1, 0, 2)),
        w_bc[0],
        jnp.transpose(w_dt[0]),
        dt_bias,
        a_log,
        d_skip,
        jnp.transpose(conv_x_weight[0], (1, 0, 2)),
        jnp.transpose(conv_x_bias, (1, 0, 2)),
        conv_bc_weight[0],
        conv_bc_bias,
        jnp.transpose(inner_gain, (1, 0, 2)),
        w_out[0].reshape(inner, width),
        x_old,
        bc_old,
        state,
    )

    def live(share, with_update):
        shares = gather_shares(share)
        sent, x_new, bc_new, stepped, decay, b_input = run_layer(shares, *layer_args)
        got = lax.all_to_all(sent, "tensor", 0, 0, tiled=True)
        factors = (stepped, decay, b_input)
        if with_update:
            factors = run_update(state, *factors)
        total = jnp.sum(got.astype(jnp.float32), axis=0)
        squares = total[:, share_cols : share_cols + 1] + total[:, share_cols + 1 : share_cols + 2]
        factor = lax.rsqrt(squares / all_channels + epsilon)
        fresh = (share.astype(jnp.float32) + total[:, :share_cols] * factor).astype(jnp.bfloat16)
        return fresh, x_new, bc_new, factors

    def rest(share, old, with_update):
        if with_update:
            return old[:3] + (run_update(state, *old[3]),)
        return old

    incoming = hidden_in
    kept = (
        jnp.zeros_like(hidden_in),
        x_old,
        bc_old,
        (
            jnp.zeros((streams, inner), jnp.float32),
            jnp.zeros((streams, heads), jnp.float32),
            jnp.zeros((streams, both // 2), jnp.float32),
        ),
    )
    for tick in range(section_count):
        last = tick + 1 == section_count
        kept = lax.cond(
            section_at == tick,
            lambda share, old, last=last: live(share, last),
            lambda share, old, last=last: rest(share, old, last),
            incoming,
            kept,
        )
        if not last:
            ring = [(at, (at + 1) % section_count) for at in range(section_count)]
            incoming = lax.ppermute(kept[0], "section", ring)
    section_share, x_new, bc_new, state_new = kept
    return (
        section_share[None],
        jnp.transpose(x_new, (2, 0, 1, 3))[None],
        jnp.transpose(bc_new, (1, 0, 2))[None],
        state_new.reshape(ssm_state.shape),
    )


def solution(mesh):
    placed = (
        P(None, "tensor"),
        P("section", None),
        P("section", None, "tensor", None),
        P("section", None, None),
        P("section", None, "tensor"),
        P("section", "tensor"),
        P("section", "tensor"),
        P("section", "tensor"),
        P("section", None, "tensor", None),
        P("section", "tensor", None),
        P("section", None, None),
        P("section", None),
        P("section", "tensor", None),
        P("section", "tensor", None, None),
        P("section", None, None, "tensor", None),
        P("section", None, None, None),
        P("section", None, "tensor", None, None),
    )
    return jax.shard_map(
        shards,
        mesh=mesh,
        in_specs=placed,
        out_specs=(
            P("section", None, "tensor"),
            P("section", None, None, "tensor", None),
            P("section", None, None, None),
            P("section", None, "tensor", None, None),
        ),
        check_vma=False,
    )
```

```python
import functools

import jax
import jax.numpy as jnp
from jax import lax
from jax.experimental import pallas as pl
from jax.experimental.pallas import tpu as pltpu
from jax.sharding import PartitionSpec as P


epsilon = 1e-05
row_block = 8
wide_lanes = 128
input_count = 16
first_flight = 2
in_flight = 6


def silu(value):
    return value / (1.0 + jnp.exp(-value))


def split_two(value):
    high = value.astype(jnp.bfloat16)
    low = (value - high.astype(jnp.float32)).astype(jnp.bfloat16)
    return high, low


def layer_math(
    shares,
    gain,
    w_heads,
    w_bc,
    w_dt,
    dt_bias,
    a_log,
    d_skip,
    conv_x_weight,
    conv_x_bias,
    conv_bc_weight,
    conv_bc_bias,
    inner_gain,
    w_out,
    conv_x_state,
    conv_bc_state,
    state,
    wait_heads,
    wait_out,
    wait_state,
    sent,
    conv_x_out,
    conv_bc_out,
    stepped_out,
    decay_out,
    b_out,
    old_part,
    gated_buf,
):
    parts, streams, share_cols = shares.shape
    heads, width, lanes = w_heads.shape
    head_size = lanes // 2
    state_size = w_bc.shape[1] // 2
    inner = heads * head_size
    blocks = streams // row_block

    wide = [shares[at].astype(jnp.float32) for at in range(parts)]
    square = sum(jnp.sum(piece * piece, axis=-1, keepdims=True) for piece in wide)
    scale = lax.rsqrt(square / width + epsilon)
    normed = jnp.concatenate(wide, axis=1) * scale * gain[...]
    normed = normed.astype(jnp.bfloat16)

    bc_fresh = jnp.dot(normed, w_bc[...], preferred_element_type=jnp.float32).astype(jnp.bfloat16)
    taps = conv_bc_weight[...]
    count = taps.shape[0]
    for tap in range(count - 2):
        conv_bc_out[tap] = conv_bc_state[tap + 1]
        conv_x_out[tap] = conv_x_state[tap + 1]
    conv_bc_out[count - 2] = bc_fresh
    bc_sum = bc_fresh.astype(jnp.float32) * taps[count - 1 : count]
    for tap in range(count - 1):
        bc_sum = bc_sum + conv_bc_state[tap].astype(jnp.float32) * taps[tap : tap + 1]
    bc_conv = silu(bc_sum + conv_bc_bias[...])
    b_input = bc_conv[:, :state_size]
    c_output = bc_conv[:, state_size:]
    b_out[...] = b_input
    overlap = jnp.sum(b_input * c_output, axis=-1, keepdims=True)
    dt_raw = lax.dot_general(
        normed, w_dt[...], (((1,), (1,)), ((), ())), preferred_element_type=jnp.float32
    )
    step_size = jax.nn.softplus(dt_raw + dt_bias[...])
    decay = jnp.exp(-step_size * jnp.exp(a_log[...]))
    decay_out[...] = decay

    c_high, c_low = split_two(c_output)
    c_high = c_high.astype(jnp.float32)
    c_low = c_low.astype(jnp.float32)
    pair_at = lax.broadcasted_iota(jnp.int32, (row_block, inner), 0) // 2
    is_odd = lax.broadcasted_iota(jnp.int32, (2 * row_block, state_size), 0) % 2 == 1
    for block in range(blocks):
        wait_state(block)
        first = block * row_block
        rows = slice(first, first + row_block)
        stacked = jnp.concatenate([c_high[rows], c_low[rows]], axis=0)
        both = jnp.concatenate(
            [jnp.where(is_odd, 0.0, stacked), jnp.where(is_odd, stacked, 0.0)], axis=1
        ).astype(jnp.bfloat16)
        kept = jnp.zeros((row_block, inner), jnp.float32)
        for pair in range(row_block // 2):
            at = first + 2 * pair
            product = lax.dot_general(
                both,
                jnp.concatenate([state[at], state[at + 1]], axis=1),
                (((1,), (1,)), ((), ())),
                preferred_element_type=jnp.float32,
            )
            kept = jnp.where(pair_at == pair, product[:row_block] + product[row_block:], kept)
        old_part[first : first + row_block, :] = kept

    squares = jnp.zeros((streams, 1), jnp.float32)
    for first in range(0, heads, 2):
        group = range(first, min(first + 2, heads))
        for head in group:
            wait_heads(head)

        def side(pieces):
            pieces = list(pieces)
            return pieces[0] if len(pieces) == 1 else jnp.concatenate(pieces, axis=1)

        def spread(table):
            return side(
                jnp.broadcast_to(table[:, head : head + 1], (streams, head_size)) for head in group
            )

        zx = jnp.dot(
            normed, side(w_heads[head] for head in group), preferred_element_type=jnp.float32
        )
        gate = side(zx[:, at * lanes : at * lanes + head_size] for at in range(len(group)))
        x_wide = side(zx[:, at * lanes + head_size : (at + 1) * lanes] for at in range(len(group)))
        x_fresh = x_wide.astype(jnp.bfloat16).astype(jnp.float32)
        for at, head in enumerate(group):
            fresh = x_fresh[:, at * head_size : (at + 1) * head_size]
            conv_x_out[count - 2, head] = fresh.astype(jnp.bfloat16)
        taps = side(conv_x_weight[head] for head in group)
        x_sum = x_fresh * taps[count - 1 : count]
        for tap in range(count - 1):
            older = side(conv_x_state[tap, head].astype(jnp.float32) for head in group)
            x_sum = x_sum + older * taps[tap : tap + 1]
        x_conv = silu(x_sum + side(conv_x_bias[head] for head in group))
        stepped = x_conv * spread(step_size)
        span = slice(first * head_size, (first + len(group)) * head_size)
        stepped_out[:, span] = stepped
        y_out = (
            spread(decay) * old_part[:, span]
            + stepped * overlap
            + side(
                jnp.broadcast_to(d_skip[:, head : head + 1], (1, head_size)) for head in group
            )
            * x_conv
        )
        gated = y_out * silu(gate)
        squares = squares + jnp.sum(gated * gated, axis=-1, keepdims=True)
        gated_buf[:, span] = gated * side(inner_gain[head] for head in group)

    scaled = gated_buf[...].astype(jnp.bfloat16)
    wait_out()
    partial = jnp.dot(scaled, w_out[...], preferred_element_type=jnp.float32)
    tail_cols = sent.shape[2] - share_cols
    high, low = split_two(squares)
    lane_at = lax.broadcasted_iota(jnp.int32, (streams, tail_cols), 1)
    tail = jnp.where(
        lane_at == 0,
        high.astype(jnp.float32),
        jnp.where(lane_at == 1, low.astype(jnp.float32), 0.0),
    )
    for at in range(parts):
        piece = partial[:, at * share_cols : (at + 1) * share_cols]
        sent[at] = jnp.concatenate([piece, tail], axis=1).astype(jnp.bfloat16)


def first_body(shares, *refs):
    inputs = refs[:input_count]
    outputs = refs[input_count : input_count + 6]
    buffers = refs[input_count + 6 : 2 * input_count + 6]
    small_sem, heads_sem, out_sem, state_sem, old_part, gated_buf = refs[2 * input_count + 6 :]
    heads = inputs[1].shape[0]
    blocks = inputs[-1].shape[0] // row_block
    large = (1, 12, input_count - 1)

    def rows(block):
        return pl.ds(block * row_block, row_block)

    small_copies = [
        pltpu.make_async_copy(inputs[at], buffers[at], small_sem.at[at])
        for at in range(input_count)
        if at not in large
    ]
    state_copies = [
        pltpu.make_async_copy(inputs[-1].at[rows(at)], buffers[-1].at[rows(at)], state_sem.at[at])
        for at in range(blocks)
    ]
    head_copies = [
        pltpu.make_async_copy(inputs[1].at[at], buffers[1].at[at], heads_sem.at[at])
        for at in range(heads)
    ]
    out_copy = pltpu.make_async_copy(inputs[12], buffers[12], out_sem)
    for copy in small_copies:
        copy.start()
    ordered = state_copies + head_copies + [out_copy]
    for copy in ordered[:first_flight]:
        copy.start()
    for copy in small_copies:
        copy.wait()
    for copy in ordered[first_flight:in_flight]:
        copy.start()

    def arrive(at):
        ordered[at].wait()
        if at + in_flight < len(ordered):
            ordered[at + in_flight].start()

    layer_math(
        shares,
        *buffers,
        lambda head: arrive(blocks + head),
        lambda: arrive(blocks + heads),
        arrive,
        *outputs,
        old_part,
        gated_buf,
    )


def stage_body(live, place, *refs):
    inputs = refs[:input_count]
    outputs = refs[input_count : 2 * input_count]
    sems = refs[2 * input_count]

    @pl.when(live[0] == 1)
    def _():
        copies = [
            pltpu.make_async_copy(inputs[at], outputs[at], sems.at[at])
            for at in range(input_count)
        ]
        for copy in copies:
            copy.start()
        for copy in copies:
            copy.wait()


def layer_body(live, place, *refs):
    shares, old_part, gated_buf = refs[-3:]
    parts = shares.shape[0]
    arrived = refs[:parts]
    inputs = refs[parts : parts + input_count]
    older = refs[parts + input_count : parts + input_count + 5]
    sent = refs[parts + input_count + 5]
    newer = refs[parts + input_count + 6 : -3]

    @pl.when(live[0] == 1)
    def _():
        for step in range(parts):
            shares[lax.rem(place[0] + parts - step, parts)] = arrived[step][...]
        def ready(*_):
            return None

        layer_math(shares, *inputs, ready, ready, ready, sent, *newer, old_part, gated_buf)

    @pl.when(live[0] == 0)
    def _():
        for source, target in zip(older, newer):
            target[...] = source[...]


def update_body(old, stepped, decay, b_input, out, state, fresh_buf, in_sems, sems):
    streams, inner, size = state.shape
    heads = decay.shape[1]
    head_size = inner // heads
    blocks = streams // row_block
    chunk_cols = wide_lanes if inner % wide_lanes == 0 else head_size

    def enter(block):
        rows = pl.ds(block * row_block, row_block)
        return pltpu.make_async_copy(old.at[rows], state.at[rows], in_sems.at[block])

    def leave(block):
        rows = pl.ds(block * row_block, row_block)
        return pltpu.make_async_copy(fresh_buf.at[rows], out.at[rows], sems.at[block])

    def step(block, carry):
        first = pl.multiple_of(block * row_block, row_block)
        enter(block).wait()

        @pl.when(block + in_flight < blocks)
        def _():
            enter(block + in_flight).start()

        stepped_rows = stepped[pl.ds(first, row_block), :]
        faded_rows = decay[pl.ds(first, row_block), :]
        b_rows = b_input[pl.ds(first, row_block), :]
        for row in range(row_block):
            b_row = jnp.broadcast_to(b_rows[row : row + 1], (head_size, size))
            for chunk in range(0, inner, chunk_cols):
                line = stepped_rows[row : row + 1, chunk : chunk + chunk_cols]
                columns = jnp.transpose(jnp.broadcast_to(line, (size, chunk_cols)))
                for at in range(0, chunk_cols, head_size):
                    head = (chunk + at) // head_size
                    span = slice(chunk + at, chunk + at + head_size)
                    faded = jnp.broadcast_to(
                        faded_rows[row : row + 1, head : head + 1], (head_size, size)
                    )
                    fresh = (
                        faded * state[first + row, span].astype(jnp.float32)
                        + columns[at : at + head_size] * b_row
                    )
                    fresh_buf[first + row, span] = fresh.astype(jnp.bfloat16)
        leave(block).start()
        return carry

    for block in range(min(in_flight, blocks)):
        enter(block).start()
    lax.fori_loop(0, blocks, step, 0)
    for block in range(blocks):
        leave(block).wait()


def whole(memory=pltpu.VMEM):
    return pl.BlockSpec(memory_space=memory)


def run_first(*operands):
    shares, gain, w_heads, w_bc, w_dt = operands[:5]
    w_out, conv_x_state, conv_bc_state, state = operands[13:]
    parts, streams, share_cols = shares.shape
    heads, width, lanes = w_heads.shape
    head_size = lanes // 2
    inner = heads * head_size
    both = w_bc.shape[1]
    sent_cols = -(-(share_cols + 2) // wide_lanes) * wide_lanes
    flops = 2 * streams * (width * (heads * lanes + both + inner)) + 2 * state.size
    moved = 2 * (w_heads.size + w_bc.size + w_out.size + state.size)
    return pl.pallas_call(
        first_body,
        in_specs=[whole()] + [whole(pltpu.HBM) for _ in operands[1:]],
        out_specs=tuple(whole() for _ in range(6)),
        out_shape=(
            jax.ShapeDtypeStruct((parts, streams, sent_cols), jnp.bfloat16),
            jax.ShapeDtypeStruct(conv_x_state.shape, jnp.bfloat16),
            jax.ShapeDtypeStruct(conv_bc_state.shape, jnp.bfloat16),
            jax.ShapeDtypeStruct((streams, inner), jnp.float32),
            jax.ShapeDtypeStruct((streams, heads), jnp.float32),
            jax.ShapeDtypeStruct((streams, both // 2), jnp.float32),
        ),
        scratch_shapes=[pltpu.VMEM(operand.shape, operand.dtype) for operand in operands[1:]]
        + [
            pltpu.SemaphoreType.DMA((input_count,)),
            pltpu.SemaphoreType.DMA((heads,)),
            pltpu.SemaphoreType.DMA(()),
            pltpu.SemaphoreType.DMA((streams // row_block,)),
            pltpu.VMEM((streams, inner), jnp.float32),
            pltpu.VMEM((streams, inner), jnp.float32),
        ],
        compiler_params=pltpu.CompilerParams(vmem_limit_bytes=44 * 1024 * 1024),
        cost_estimate=pl.CostEstimate(flops=flops, transcendentals=0, bytes_accessed=moved),
        name="first_layer",
    )(*operands)


def run_stage(live, place, *operands):
    moved = sum(operand.size * operand.dtype.itemsize for operand in operands)
    return pl.pallas_call(
        stage_body,
        in_specs=[whole(pltpu.SMEM)] * 2 + [whole(pltpu.HBM) for _ in operands],
        out_specs=tuple(whole() for _ in operands),
        out_shape=tuple(pltpu.VMEM(operand.shape, operand.dtype) for operand in operands),
        scratch_shapes=[pltpu.SemaphoreType.DMA((input_count,))],
        compiler_params=pltpu.CompilerParams(vmem_limit_bytes=1024 * 1024),
        cost_estimate=pl.CostEstimate(flops=40 * moved, transcendentals=0, bytes_accessed=moved),
        name="stage",
    )(live, place, *operands)


def run_layer(live, place, arrived, staged, older):
    parts = len(arrived)
    streams, share_cols = arrived[0].shape
    sent_cols = -(-(share_cols + 2) // wide_lanes) * wide_lanes
    inner = older[2].shape[1]
    outs = (jax.ShapeDtypeStruct((parts, streams, sent_cols), jnp.bfloat16),) + tuple(
        jax.ShapeDtypeStruct(value.shape, value.dtype) for value in older
    )
    moved = sum(operand.size for operand in staged)
    return pl.pallas_call(
        layer_body,
        in_specs=[whole(pltpu.SMEM)] * 2 + [whole() for _ in range(parts + len(staged) + len(older))],
        out_specs=tuple(whole() for _ in outs),
        out_shape=outs,
        scratch_shapes=[
            pltpu.VMEM((parts, streams, share_cols), arrived[0].dtype),
            pltpu.VMEM((streams, inner), jnp.float32),
            pltpu.VMEM((streams, inner), jnp.float32),
        ],
        compiler_params=pltpu.CompilerParams(vmem_limit_bytes=10 * 1024 * 1024),
        cost_estimate=pl.CostEstimate(
            flops=2 * streams * moved, transcendentals=0, bytes_accessed=2 * moved
        ),
        name="layer",
    )(live, place, *arrived, *staged, *older)


def run_update(state, stepped, decay, b_input):
    blocks = state.shape[0] // row_block
    return pl.pallas_call(
        update_body,
        in_specs=[whole(pltpu.HBM)] + [whole() for _ in range(3)],
        out_specs=whole(pltpu.HBM),
        out_shape=jax.ShapeDtypeStruct(state.shape, state.dtype),
        scratch_shapes=[
            pltpu.VMEM(state.shape, state.dtype),
            pltpu.VMEM(state.shape, state.dtype),
            pltpu.SemaphoreType.DMA((blocks,)),
            pltpu.SemaphoreType.DMA((blocks,)),
        ],
        compiler_params=pltpu.CompilerParams(vmem_limit_bytes=24 * 1024 * 1024),
        cost_estimate=pl.CostEstimate(
            flops=40 * state.size, transcendentals=0, bytes_accessed=4 * state.size
        ),
        name="update",
    )(state, stepped, decay, b_input)


def gather_shares(share):
    count = lax.axis_size("tensor")
    spread = jnp.broadcast_to(share[None], (count,) + share.shape)
    return lax.all_to_all(spread, "tensor", 0, 0, tiled=True)


def hand_over(share, source, target, parts):
    return [
        lax.ppermute(
            share,
            ("section", "tensor"),
            [(source * parts + at, target * parts + (at + step) % parts) for at in range(parts)],
        )
        for step in range(parts)
    ]


def shards(
    hidden_in,
    pre_gain,
    w_zx,
    w_bc,
    w_dt,
    dt_bias,
    a_log,
    d_skip,
    conv_x_weight,
    conv_x_bias,
    conv_bc_weight,
    conv_bc_bias,
    inner_gain,
    w_out,
    conv_x_state,
    conv_bc_state,
    ssm_state,
):
    section_count = lax.axis_size("section")
    tensor_count = lax.axis_size("tensor")
    section_at = lax.axis_index("section")
    streams, share_cols = hidden_in.shape
    width = w_zx.shape[1]
    heads = w_zx.shape[2]
    head_size = w_zx.shape[3] // 2
    both = w_bc.shape[2]
    inner = heads * head_size
    all_channels = inner * tensor_count
    state = ssm_state[0].reshape(streams, inner, both // 2)
    x_old = jnp.transpose(conv_x_state[0], (1, 2, 0, 3))
    bc_old = jnp.transpose(conv_bc_state[0], (1, 0, 2))
    layer_args = (
        pre_gain,
        jnp.transpose(w_zx[0], (1, 0, 2)),
        w_bc[0],
        jnp.transpose(w_dt[0]),
        dt_bias,
        a_log,
        d_skip,
        jnp.transpose(conv_x_weight[0], (1, 0, 2)),
        jnp.transpose(conv_x_bias, (1, 0, 2)),
        conv_bc_weight[0],
        conv_bc_bias,
        jnp.transpose(inner_gain, (1, 0, 2)),
        w_out[0].reshape(inner, width),
        x_old,
        bc_old,
        state,
    )

    def reduced(sent, share, factors, last):
        got = lax.all_to_all(sent, "tensor", 0, 0, tiled=True)
        if last:
            factors = run_update(state, *factors)
        total = jnp.sum(got.astype(jnp.float32), axis=0)
        squares = total[:, share_cols : share_cols + 1] + total[:, share_cols + 1 : share_cols + 2]
        factor = lax.rsqrt(squares / all_channels + epsilon)
        fresh = (share.astype(jnp.float32) + total[:, :share_cols] * factor).astype(jnp.bfloat16)
        return fresh, factors

    older = (
        x_old,
        bc_old,
        jnp.zeros((streams, inner), jnp.float32),
        jnp.zeros((streams, heads), jnp.float32),
        jnp.zeros((streams, both // 2), jnp.float32),
    )
    def first_live(share, older):
        sent, *newer = run_first(gather_shares(share), *layer_args)
        return reduced(sent, share, (), False)[0], tuple(newer)

    section_share, older = lax.cond(
        section_at == 0, first_live, lambda share, older: (share, older), hidden_in, older
    )
    tensor_at = lax.axis_index("tensor").astype(jnp.int32)
    for tick in range(1, section_count):
        last = tick + 1 == section_count
        section_share, here, place = lax.optimization_barrier(
            (section_share, section_at, tensor_at)
        )
        is_live = here == tick
        live = is_live.astype(jnp.int32)[None]
        place = place[None]
        arrived = hand_over(section_share, tick - 1, tick, tensor_count)
        staged = run_stage(live, place, *layer_args)
        sent, *older = run_layer(live, place, arrived, staged, older)
        factors = tuple(older[2:]) if last else ()

        def rest(sent, own, kept, factors, last=last):
            return kept, run_update(state, *factors) if last else factors

        section_share, state_new = lax.cond(
            is_live,
            lambda sent, own, kept, factors, last=last: reduced(sent, own, factors, last),
            rest,
            sent,
            arrived[0],
            section_share,
            factors,
        )
    x_new, bc_new = older[:2]
    return (
        section_share[None],
        jnp.transpose(x_new, (2, 0, 1, 3))[None],
        jnp.transpose(bc_new, (1, 0, 2))[None],
        state_new.reshape(ssm_state.shape),
    )


def solution(mesh):
    placed = (
        P(None, "tensor"),
        P("section", None),
        P("section", None, "tensor", None),
        P("section", None, None),
        P("section", None, "tensor"),
        P("section", "tensor"),
        P("section", "tensor"),
        P("section", "tensor"),
        P("section", None, "tensor", None),
        P("section", "tensor", None),
        P("section", None, None),
        P("section", None),
        P("section", "tensor", None),
        P("section", "tensor", None, None),
        P("section", None, None, "tensor", None),
        P("section", None, None, None),
        P("section", None, "tensor", None, None),
    )
    return jax.shard_map(
        shards,
        mesh=mesh,
        in_specs=placed,
        out_specs=(
            P("section", None, "tensor"),
            P("section", None, None, "tensor", None),
            P("section", None, None, None),
            P("section", None, "tensor", None, None),
        ),
        check_vma=False,
    )
```

```python
import functools

import jax
import jax.numpy as jnp
from jax import lax
from jax.experimental import pallas as pl
from jax.experimental.pallas import tpu as pltpu
from jax.sharding import PartitionSpec as P


epsilon = 1e-05
row_block = 8
wide_lanes = 128
ring_steps = 2
input_count = 16
first_flight = 2
in_flight = 6


def silu(value):
    return value / (1.0 + jnp.exp(-value))


def split_two(value):
    high = value.astype(jnp.bfloat16)
    low = (value - high.astype(jnp.float32)).astype(jnp.bfloat16)
    return high, low


def layer_math(
    shares,
    gain,
    w_heads,
    w_bc,
    w_dt,
    dt_bias,
    a_log,
    d_skip,
    conv_x_weight,
    conv_x_bias,
    conv_bc_weight,
    conv_bc_bias,
    inner_gain,
    w_out,
    conv_x_state,
    conv_bc_state,
    state,
    wait_heads,
    wait_out,
    wait_state,
    sent,
    conv_x_out,
    conv_bc_out,
    stepped_out,
    decay_out,
    b_out,
    old_part,
    gated_buf,
):
    parts, streams, share_cols = shares.shape
    heads, width, lanes = w_heads.shape
    head_size = lanes // 2
    state_size = w_bc.shape[1] // 2
    inner = heads * head_size
    blocks = streams // row_block

    wide = [shares[at].astype(jnp.float32) for at in range(parts)]
    square = sum(jnp.sum(piece * piece, axis=-1, keepdims=True) for piece in wide)
    scale = lax.rsqrt(square / width + epsilon)
    normed = jnp.concatenate(wide, axis=1) * scale * gain[...]
    normed = normed.astype(jnp.bfloat16)

    bc_fresh = jnp.dot(normed, w_bc[...], preferred_element_type=jnp.float32).astype(jnp.bfloat16)
    taps = conv_bc_weight[...]
    count = taps.shape[0]
    for tap in range(count - 2):
        conv_bc_out[tap] = conv_bc_state[tap + 1]
        conv_x_out[tap] = conv_x_state[tap + 1]
    conv_bc_out[count - 2] = bc_fresh
    bc_sum = bc_fresh.astype(jnp.float32) * taps[count - 1 : count]
    for tap in range(count - 1):
        bc_sum = bc_sum + conv_bc_state[tap].astype(jnp.float32) * taps[tap : tap + 1]
    bc_conv = silu(bc_sum + conv_bc_bias[...])
    b_input = bc_conv[:, :state_size]
    c_output = bc_conv[:, state_size:]
    b_out[...] = b_input
    overlap = jnp.sum(b_input * c_output, axis=-1, keepdims=True)
    dt_raw = lax.dot_general(
        normed, w_dt[...], (((1,), (1,)), ((), ())), preferred_element_type=jnp.float32
    )
    step_size = jax.nn.softplus(dt_raw + dt_bias[...])
    decay = jnp.exp(-step_size * jnp.exp(a_log[...]))
    decay_out[...] = decay

    c_high, c_low = split_two(c_output)
    c_high = c_high.astype(jnp.float32)
    c_low = c_low.astype(jnp.float32)
    pair_at = lax.broadcasted_iota(jnp.int32, (row_block, inner), 0) // 2
    is_odd = lax.broadcasted_iota(jnp.int32, (2 * row_block, state_size), 0) % 2 == 1
    for block in range(blocks):
        wait_state(block)
        first = block * row_block
        rows = slice(first, first + row_block)
        stacked = jnp.concatenate([c_high[rows], c_low[rows]], axis=0)
        both = jnp.concatenate(
            [jnp.where(is_odd, 0.0, stacked), jnp.where(is_odd, stacked, 0.0)], axis=1
        ).astype(jnp.bfloat16)
        kept = jnp.zeros((row_block, inner), jnp.float32)
        for pair in range(row_block // 2):
            at = first + 2 * pair
            product = lax.dot_general(
                both,
                jnp.concatenate([state[at], state[at + 1]], axis=1),
                (((1,), (1,)), ((), ())),
                preferred_element_type=jnp.float32,
            )
            kept = jnp.where(pair_at == pair, product[:row_block] + product[row_block:], kept)
        old_part[first : first + row_block, :] = kept

    squares = jnp.zeros((streams, 1), jnp.float32)
    for first in range(0, heads, 2):
        group = range(first, min(first + 2, heads))
        for head in group:
            wait_heads(head)

        def side(pieces):
            pieces = list(pieces)
            return pieces[0] if len(pieces) == 1 else jnp.concatenate(pieces, axis=1)

        def spread(table):
            return side(
                jnp.broadcast_to(table[:, head : head + 1], (streams, head_size)) for head in group
            )

        zx = jnp.dot(
            normed, side(w_heads[head] for head in group), preferred_element_type=jnp.float32
        )
        gate = side(zx[:, at * lanes : at * lanes + head_size] for at in range(len(group)))
        x_wide = side(zx[:, at * lanes + head_size : (at + 1) * lanes] for at in range(len(group)))
        x_fresh = x_wide.astype(jnp.bfloat16).astype(jnp.float32)
        for at, head in enumerate(group):
            fresh = x_fresh[:, at * head_size : (at + 1) * head_size]
            conv_x_out[count - 2, head] = fresh.astype(jnp.bfloat16)
        taps = side(conv_x_weight[head] for head in group)
        x_sum = x_fresh * taps[count - 1 : count]
        for tap in range(count - 1):
            older = side(conv_x_state[tap, head].astype(jnp.float32) for head in group)
            x_sum = x_sum + older * taps[tap : tap + 1]
        x_conv = silu(x_sum + side(conv_x_bias[head] for head in group))
        stepped = x_conv * spread(step_size)
        span = slice(first * head_size, (first + len(group)) * head_size)
        stepped_out[:, span] = stepped
        y_out = (
            spread(decay) * old_part[:, span]
            + stepped * overlap
            + side(
                jnp.broadcast_to(d_skip[:, head : head + 1], (1, head_size)) for head in group
            )
            * x_conv
        )
        gated = y_out * silu(gate)
        squares = squares + jnp.sum(gated * gated, axis=-1, keepdims=True)
        gated_buf[:, span] = gated * side(inner_gain[head] for head in group)

    scaled = gated_buf[...].astype(jnp.bfloat16)
    wait_out()
    partial = jnp.dot(scaled, w_out[...], preferred_element_type=jnp.float32)
    tail_cols = sent.shape[2] - share_cols
    high, low = split_two(squares)
    lane_at = lax.broadcasted_iota(jnp.int32, (streams, tail_cols), 1)
    tail = jnp.where(
        lane_at == 0,
        high.astype(jnp.float32),
        jnp.where(lane_at == 1, low.astype(jnp.float32), 0.0),
    )
    for at in range(parts):
        piece = partial[:, at * share_cols : (at + 1) * share_cols]
        sent[at] = jnp.concatenate([piece, tail], axis=1).astype(jnp.bfloat16)


def first_body(shares, *refs):
    inputs = refs[:input_count]
    outputs = refs[input_count : input_count + 6]
    buffers = refs[input_count + 6 : 2 * input_count + 6]
    small_sem, heads_sem, out_sem, state_sem, old_part, gated_buf = refs[2 * input_count + 6 :]
    heads = inputs[1].shape[0]
    blocks = inputs[-1].shape[0] // row_block
    large = (1, 12, input_count - 1)

    def rows(block):
        return pl.ds(block * row_block, row_block)

    small_copies = [
        pltpu.make_async_copy(inputs[at], buffers[at], small_sem.at[at])
        for at in range(input_count)
        if at not in large
    ]
    state_copies = [
        pltpu.make_async_copy(inputs[-1].at[rows(at)], buffers[-1].at[rows(at)], state_sem.at[at])
        for at in range(blocks)
    ]
    head_copies = [
        pltpu.make_async_copy(inputs[1].at[at], buffers[1].at[at], heads_sem.at[at])
        for at in range(heads)
    ]
    out_copy = pltpu.make_async_copy(inputs[12], buffers[12], out_sem)
    for copy in small_copies:
        copy.start()
    ordered = state_copies + head_copies + [out_copy]
    for copy in ordered[:first_flight]:
        copy.start()
    for copy in small_copies:
        copy.wait()
    for copy in ordered[first_flight:in_flight]:
        copy.start()

    def arrive(at):
        ordered[at].wait()
        if at + in_flight < len(ordered):
            ordered[at + in_flight].start()

    layer_math(
        shares,
        *buffers,
        lambda head: arrive(blocks + head),
        lambda: arrive(blocks + heads),
        arrive,
        *outputs,
        old_part,
        gated_buf,
    )


def stage_body(live, place, *refs):
    inputs = refs[:input_count]
    outputs = refs[input_count : 2 * input_count]
    sems = refs[2 * input_count]

    @pl.when(live[0] == 1)
    def _():
        copies = [
            pltpu.make_async_copy(inputs[at], outputs[at], sems.at[at])
            for at in range(input_count)
        ]
        for copy in copies:
            copy.start()
        for copy in copies:
            copy.wait()


def layer_body(live, place, *refs):
    shares, old_part, gated_buf = refs[-3:]
    parts = shares.shape[0]
    arrived = refs[:parts]
    inputs = refs[parts : parts + input_count]
    older = refs[parts + input_count : parts + input_count + 5]
    sent = refs[parts + input_count + 5]
    newer = refs[parts + input_count + 6 : -3]

    @pl.when(live[0] == 1)
    def _():
        for step in range(parts):
            shares[lax.rem(place[0] + parts - step, parts)] = arrived[step][...]
        def ready(*_):
            return None

        layer_math(shares, *inputs, ready, ready, ready, sent, *newer, old_part, gated_buf)

    @pl.when(live[0] == 0)
    def _():
        for source, target in zip(older, newer):
            target[...] = source[...]


def update_body(old, stepped, decay, b_input, out, state, fresh_buf, in_sems, sems):
    streams, inner, size = state.shape
    heads = decay.shape[1]
    head_size = inner // heads
    blocks = streams // row_block
    chunk_cols = wide_lanes if inner % wide_lanes == 0 else head_size

    def enter(block):
        rows = pl.ds(block * row_block, row_block)
        return pltpu.make_async_copy(old.at[rows], state.at[rows], in_sems.at[block])

    def leave(block):
        rows = pl.ds(block * row_block, row_block)
        return pltpu.make_async_copy(fresh_buf.at[rows], out.at[rows], sems.at[block])

    def step(block, carry):
        first = pl.multiple_of(block * row_block, row_block)
        enter(block).wait()

        @pl.when(block + in_flight < blocks)
        def _():
            enter(block + in_flight).start()

        stepped_rows = stepped[pl.ds(first, row_block), :]
        faded_rows = decay[pl.ds(first, row_block), :]
        b_rows = b_input[pl.ds(first, row_block), :]
        for row in range(row_block):
            b_row = jnp.broadcast_to(b_rows[row : row + 1], (head_size, size))
            for chunk in range(0, inner, chunk_cols):
                line = stepped_rows[row : row + 1, chunk : chunk + chunk_cols]
                columns = jnp.transpose(jnp.broadcast_to(line, (size, chunk_cols)))
                for at in range(0, chunk_cols, head_size):
                    head = (chunk + at) // head_size
                    span = slice(chunk + at, chunk + at + head_size)
                    faded = jnp.broadcast_to(
                        faded_rows[row : row + 1, head : head + 1], (head_size, size)
                    )
                    fresh = (
                        faded * state[first + row, span].astype(jnp.float32)
                        + columns[at : at + head_size] * b_row
                    )
                    fresh_buf[first + row, span] = fresh.astype(jnp.bfloat16)
        leave(block).start()
        return carry

    for block in range(min(in_flight, blocks)):
        enter(block).start()
    lax.fori_loop(0, blocks, step, 0)
    for block in range(blocks):
        leave(block).wait()


def whole(memory=pltpu.VMEM):
    return pl.BlockSpec(memory_space=memory)


def run_first(*operands):
    shares, gain, w_heads, w_bc, w_dt = operands[:5]
    w_out, conv_x_state, conv_bc_state, state = operands[13:]
    parts, streams, share_cols = shares.shape
    heads, width, lanes = w_heads.shape
    head_size = lanes // 2
    inner = heads * head_size
    both = w_bc.shape[1]
    sent_cols = -(-(share_cols + 2) // wide_lanes) * wide_lanes
    flops = 2 * streams * (width * (heads * lanes + both + inner)) + 2 * state.size
    moved = 2 * (w_heads.size + w_bc.size + w_out.size + state.size)
    return pl.pallas_call(
        first_body,
        in_specs=[whole()] + [whole(pltpu.HBM) for _ in operands[1:]],
        out_specs=tuple(whole() for _ in range(6)),
        out_shape=(
            jax.ShapeDtypeStruct((parts, streams, sent_cols), jnp.bfloat16),
            jax.ShapeDtypeStruct(conv_x_state.shape, jnp.bfloat16),
            jax.ShapeDtypeStruct(conv_bc_state.shape, jnp.bfloat16),
            jax.ShapeDtypeStruct((streams, inner), jnp.float32),
            jax.ShapeDtypeStruct((streams, heads), jnp.float32),
            jax.ShapeDtypeStruct((streams, both // 2), jnp.float32),
        ),
        scratch_shapes=[pltpu.VMEM(operand.shape, operand.dtype) for operand in operands[1:]]
        + [
            pltpu.SemaphoreType.DMA((input_count,)),
            pltpu.SemaphoreType.DMA((heads,)),
            pltpu.SemaphoreType.DMA(()),
            pltpu.SemaphoreType.DMA((streams // row_block,)),
            pltpu.VMEM((streams, inner), jnp.float32),
            pltpu.VMEM((streams, inner), jnp.float32),
        ],
        compiler_params=pltpu.CompilerParams(vmem_limit_bytes=44 * 1024 * 1024),
        cost_estimate=pl.CostEstimate(flops=flops, transcendentals=0, bytes_accessed=moved),
        name="first_layer",
    )(*operands)


def run_stage(live, place, *operands):
    moved = sum(operand.size * operand.dtype.itemsize for operand in operands)
    return pl.pallas_call(
        stage_body,
        in_specs=[whole(pltpu.SMEM)] * 2 + [whole(pltpu.HBM) for _ in operands],
        out_specs=tuple(whole() for _ in operands),
        out_shape=tuple(pltpu.VMEM(operand.shape, operand.dtype) for operand in operands),
        scratch_shapes=[pltpu.SemaphoreType.DMA((input_count,))],
        compiler_params=pltpu.CompilerParams(vmem_limit_bytes=1024 * 1024),
        cost_estimate=pl.CostEstimate(flops=40 * moved, transcendentals=0, bytes_accessed=moved),
        name="stage",
    )(live, place, *operands)


def run_layer(live, place, arrived, staged, older):
    parts = len(arrived)
    streams, share_cols = arrived[0].shape
    sent_cols = -(-(share_cols + 2) // wide_lanes) * wide_lanes
    inner = older[2].shape[1]
    outs = (jax.ShapeDtypeStruct((parts, streams, sent_cols), jnp.bfloat16),) + tuple(
        jax.ShapeDtypeStruct(value.shape, value.dtype) for value in older
    )
    moved = sum(operand.size for operand in staged)
    return pl.pallas_call(
        layer_body,
        in_specs=[whole(pltpu.SMEM)] * 2 + [whole() for _ in range(parts + len(staged) + len(older))],
        out_specs=tuple(whole() for _ in outs),
        out_shape=outs,
        scratch_shapes=[
            pltpu.VMEM((parts, streams, share_cols), arrived[0].dtype),
            pltpu.VMEM((streams, inner), jnp.float32),
            pltpu.VMEM((streams, inner), jnp.float32),
        ],
        compiler_params=pltpu.CompilerParams(vmem_limit_bytes=10 * 1024 * 1024),
        cost_estimate=pl.CostEstimate(
            flops=2 * streams * moved, transcendentals=0, bytes_accessed=2 * moved
        ),
        name="layer",
    )(live, place, *arrived, *staged, *older)


def run_update(state, stepped, decay, b_input):
    blocks = state.shape[0] // row_block
    return pl.pallas_call(
        update_body,
        in_specs=[whole(pltpu.HBM)] + [whole() for _ in range(3)],
        out_specs=whole(pltpu.HBM),
        out_shape=jax.ShapeDtypeStruct(state.shape, state.dtype),
        scratch_shapes=[
            pltpu.VMEM(state.shape, state.dtype),
            pltpu.VMEM(state.shape, state.dtype),
            pltpu.SemaphoreType.DMA((blocks,)),
            pltpu.SemaphoreType.DMA((blocks,)),
        ],
        compiler_params=pltpu.CompilerParams(vmem_limit_bytes=24 * 1024 * 1024),
        cost_estimate=pl.CostEstimate(
            flops=40 * state.size, transcendentals=0, bytes_accessed=4 * state.size
        ),
        name="update",
    )(state, stepped, decay, b_input)


def gather_shares(share):
    count = lax.axis_size("tensor")
    spread = jnp.broadcast_to(share[None], (count,) + share.shape)
    return lax.all_to_all(spread, "tensor", 0, 0, tiled=True)


def hand_over(share, source, target, parts, sections):
    def pairs(step):
        moves = [(source, target)]
        if step >= parts - ring_steps:
            moves = [(at, (at + 1) % sections) for at in range(sections)]
        return [
            (start * parts + at, end * parts + (at + step) % parts)
            for start, end in moves
            for at in range(parts)
        ]

    return [lax.ppermute(share, ("section", "tensor"), pairs(step)) for step in range(parts)]


def shards(
    hidden_in,
    pre_gain,
    w_zx,
    w_bc,
    w_dt,
    dt_bias,
    a_log,
    d_skip,
    conv_x_weight,
    conv_x_bias,
    conv_bc_weight,
    conv_bc_bias,
    inner_gain,
    w_out,
    conv_x_state,
    conv_bc_state,
    ssm_state,
):
    section_count = lax.axis_size("section")
    tensor_count = lax.axis_size("tensor")
    section_at = lax.axis_index("section")
    streams, share_cols = hidden_in.shape
    width = w_zx.shape[1]
    heads = w_zx.shape[2]
    head_size = w_zx.shape[3] // 2
    both = w_bc.shape[2]
    inner = heads * head_size
    all_channels = inner * tensor_count
    state = ssm_state[0].reshape(streams, inner, both // 2)
    x_old = jnp.transpose(conv_x_state[0], (1, 2, 0, 3))
    bc_old = jnp.transpose(conv_bc_state[0], (1, 0, 2))
    layer_args = (
        pre_gain,
        jnp.transpose(w_zx[0], (1, 0, 2)),
        w_bc[0],
        jnp.transpose(w_dt[0]),
        dt_bias,
        a_log,
        d_skip,
        jnp.transpose(conv_x_weight[0], (1, 0, 2)),
        jnp.transpose(conv_x_bias, (1, 0, 2)),
        conv_bc_weight[0],
        conv_bc_bias,
        jnp.transpose(inner_gain, (1, 0, 2)),
        w_out[0].reshape(inner, width),
        x_old,
        bc_old,
        state,
    )

    def reduced(sent, share, factors, last):
        got = lax.all_to_all(sent, "tensor", 0, 0, tiled=True)
        if last:
            factors = run_update(state, *factors)
        total = jnp.sum(got.astype(jnp.float32), axis=0)
        squares = total[:, share_cols : share_cols + 1] + total[:, share_cols + 1 : share_cols + 2]
        factor = lax.rsqrt(squares / all_channels + epsilon)
        fresh = (share.astype(jnp.float32) + total[:, :share_cols] * factor).astype(jnp.bfloat16)
        return fresh, factors

    older = (
        x_old,
        bc_old,
        jnp.zeros((streams, inner), jnp.float32),
        jnp.zeros((streams, heads), jnp.float32),
        jnp.zeros((streams, both // 2), jnp.float32),
    )
    def first_live(share, older):
        sent, *newer = run_first(gather_shares(share), *layer_args)
        return reduced(sent, share, (), False)[0], tuple(newer)

    section_share, older = lax.cond(
        section_at == 0, first_live, lambda share, older: (share, older), hidden_in, older
    )
    tensor_at = lax.axis_index("tensor").astype(jnp.int32)
    for tick in range(1, section_count):
        last = tick + 1 == section_count
        section_share, here, place = lax.optimization_barrier(
            (section_share, section_at, tensor_at)
        )
        is_live = here == tick
        live = is_live.astype(jnp.int32)[None]
        place = place[None]
        arrived = hand_over(section_share, tick - 1, tick, tensor_count, section_count)
        staged = run_stage(live, place, *layer_args)
        sent, *older = run_layer(live, place, arrived, staged, older)
        factors = tuple(older[2:]) if last else ()

        def rest(sent, own, kept, factors, last=last):
            return kept, run_update(state, *factors) if last else factors

        section_share, state_new = lax.cond(
            is_live,
            lambda sent, own, kept, factors, last=last: reduced(sent, own, factors, last),
            rest,
            sent,
            arrived[0],
            section_share,
            factors,
        )
    x_new, bc_new = older[:2]
    return (
        section_share[None],
        jnp.transpose(x_new, (2, 0, 1, 3))[None],
        jnp.transpose(bc_new, (1, 0, 2))[None],
        state_new.reshape(ssm_state.shape),
    )


def solution(mesh):
    placed = (
        P(None, "tensor"),
        P("section", None),
        P("section", None, "tensor", None),
        P("section", None, None),
        P("section", None, "tensor"),
        P("section", "tensor"),
        P("section", "tensor"),
        P("section", "tensor"),
        P("section", None, "tensor", None),
        P("section", "tensor", None),
        P("section", None, None),
        P("section", None),
        P("section", "tensor", None),
        P("section", "tensor", None, None),
        P("section", None, None, "tensor", None),
        P("section", None, None, None),
        P("section", None, "tensor", None, None),
    )
    return jax.shard_map(
        shards,
        mesh=mesh,
        in_specs=placed,
        out_specs=(
            P("section", None, "tensor"),
            P("section", None, None, "tensor", None),
            P("section", None, None, None),
            P("section", None, "tensor", None, None),
        ),
        check_vma=False,
    )
```

```python
import functools

import jax
import jax.numpy as jnp
from jax import lax
from jax.experimental import pallas as pl
from jax.experimental.pallas import tpu as pltpu
from jax.sharding import PartitionSpec as P


epsilon = 1e-05
row_block = 8
wide_lanes = 128
ring_steps = 2
input_count = 16
first_flight = 2
in_flight = 6


def silu(value):
    return value / (1.0 + jnp.exp(-value))


def split_two(value):
    high = value.astype(jnp.bfloat16)
    low = (value - high.astype(jnp.float32)).astype(jnp.bfloat16)
    return high, low


def layer_math(
    shares,
    gain,
    w_heads,
    w_bc,
    w_dt,
    dt_bias,
    a_log,
    d_skip,
    conv_x_weight,
    conv_x_bias,
    conv_bc_weight,
    conv_bc_bias,
    inner_gain,
    w_out,
    conv_x_state,
    conv_bc_state,
    state,
    wait_heads,
    wait_out,
    wait_state,
    sent,
    conv_x_out,
    conv_bc_out,
    stepped_out,
    decay_out,
    b_out,
    old_part,
    gated_buf,
):
    parts, streams, share_cols = shares.shape
    heads, width, lanes = w_heads.shape
    head_size = lanes // 2
    state_size = w_bc.shape[1] // 2
    inner = heads * head_size
    blocks = streams // row_block

    wide = [shares[at].astype(jnp.float32) for at in range(parts)]
    square = sum(jnp.sum(piece * piece, axis=-1, keepdims=True) for piece in wide)
    scale = lax.rsqrt(square / width + epsilon)
    normed = jnp.concatenate(wide, axis=1) * scale * gain[...]
    normed = normed.astype(jnp.bfloat16)

    bc_fresh = jnp.dot(normed, w_bc[...], preferred_element_type=jnp.float32).astype(jnp.bfloat16)
    taps = conv_bc_weight[...]
    count = taps.shape[0]
    for tap in range(count - 2):
        conv_bc_out[tap] = conv_bc_state[tap + 1]
        conv_x_out[tap] = conv_x_state[tap + 1]
    conv_bc_out[count - 2] = bc_fresh
    bc_sum = bc_fresh.astype(jnp.float32) * taps[count - 1 : count]
    for tap in range(count - 1):
        bc_sum = bc_sum + conv_bc_state[tap].astype(jnp.float32) * taps[tap : tap + 1]
    bc_conv = silu(bc_sum + conv_bc_bias[...])
    b_input = bc_conv[:, :state_size]
    c_output = bc_conv[:, state_size:]
    b_out[...] = b_input
    overlap = jnp.sum(b_input * c_output, axis=-1, keepdims=True)
    dt_raw = lax.dot_general(
        normed, w_dt[...], (((1,), (1,)), ((), ())), preferred_element_type=jnp.float32
    )
    step_size = jax.nn.softplus(dt_raw + dt_bias[...])
    decay = jnp.exp(-step_size * jnp.exp(a_log[...]))
    decay_out[...] = decay

    c_high, c_low = split_two(c_output)
    c_high = c_high.astype(jnp.float32)
    c_low = c_low.astype(jnp.float32)
    pair_at = lax.broadcasted_iota(jnp.int32, (row_block, inner), 0) // 2
    is_odd = lax.broadcasted_iota(jnp.int32, (2 * row_block, state_size), 0) % 2 == 1
    for block in range(blocks):
        wait_state(block)
        first = block * row_block
        rows = slice(first, first + row_block)
        stacked = jnp.concatenate([c_high[rows], c_low[rows]], axis=0)
        both = jnp.concatenate(
            [jnp.where(is_odd, 0.0, stacked), jnp.where(is_odd, stacked, 0.0)], axis=1
        ).astype(jnp.bfloat16)
        kept = jnp.zeros((row_block, inner), jnp.float32)
        for pair in range(row_block // 2):
            at = first + 2 * pair
            product = lax.dot_general(
                both,
                jnp.concatenate([state[at], state[at + 1]], axis=1),
                (((1,), (1,)), ((), ())),
                preferred_element_type=jnp.float32,
            )
            kept = jnp.where(pair_at == pair, product[:row_block] + product[row_block:], kept)
        old_part[first : first + row_block, :] = kept

    squares = jnp.zeros((streams, 1), jnp.float32)
    for first in range(0, heads, 2):
        group = range(first, min(first + 2, heads))
        for head in group:
            wait_heads(head)

        def side(pieces):
            pieces = list(pieces)
            return pieces[0] if len(pieces) == 1 else jnp.concatenate(pieces, axis=1)

        def spread(table):
            return side(
                jnp.broadcast_to(table[:, head : head + 1], (streams, head_size)) for head in group
            )

        zx = jnp.dot(
            normed, side(w_heads[head] for head in group), preferred_element_type=jnp.float32
        )
        gate = side(zx[:, at * lanes : at * lanes + head_size] for at in range(len(group)))
        x_wide = side(zx[:, at * lanes + head_size : (at + 1) * lanes] for at in range(len(group)))
        x_fresh = x_wide.astype(jnp.bfloat16).astype(jnp.float32)
        for at, head in enumerate(group):
            fresh = x_fresh[:, at * head_size : (at + 1) * head_size]
            conv_x_out[count - 2, head] = fresh.astype(jnp.bfloat16)
        taps = side(conv_x_weight[head] for head in group)
        x_sum = x_fresh * taps[count - 1 : count]
        for tap in range(count - 1):
            older = side(conv_x_state[tap, head].astype(jnp.float32) for head in group)
            x_sum = x_sum + older * taps[tap : tap + 1]
        x_conv = silu(x_sum + side(conv_x_bias[head] for head in group))
        stepped = x_conv * spread(step_size)
        span = slice(first * head_size, (first + len(group)) * head_size)
        stepped_out[:, span] = stepped
        y_out = (
            spread(decay) * old_part[:, span]
            + stepped * overlap
            + side(
                jnp.broadcast_to(d_skip[:, head : head + 1], (1, head_size)) for head in group
            )
            * x_conv
        )
        gated = y_out * silu(gate)
        squares = squares + jnp.sum(gated * gated, axis=-1, keepdims=True)
        gated_buf[:, span] = gated * side(inner_gain[head] for head in group)

    scaled = gated_buf[...].astype(jnp.bfloat16)
    wait_out()
    partial = jnp.dot(scaled, w_out[...], preferred_element_type=jnp.float32)
    tail_cols = sent.shape[2] - share_cols
    high, low = split_two(squares)
    lane_at = lax.broadcasted_iota(jnp.int32, (streams, tail_cols), 1)
    tail = jnp.where(
        lane_at == 0,
        high.astype(jnp.float32),
        jnp.where(lane_at == 1, low.astype(jnp.float32), 0.0),
    )
    for at in range(parts):
        piece = partial[:, at * share_cols : (at + 1) * share_cols]
        sent[at] = jnp.concatenate([piece, tail], axis=1).astype(jnp.bfloat16)


def first_body(shares, *refs):
    inputs = refs[:input_count]
    outputs = refs[input_count : input_count + 6]
    buffers = refs[input_count + 6 : 2 * input_count + 6]
    small_sem, heads_sem, out_sem, state_sem, old_part, gated_buf = refs[2 * input_count + 6 :]
    heads = inputs[1].shape[0]
    blocks = inputs[-1].shape[0] // row_block
    large = (1, 12, input_count - 1)

    def rows(block):
        return pl.ds(block * row_block, row_block)

    small_copies = [
        pltpu.make_async_copy(inputs[at], buffers[at], small_sem.at[at])
        for at in range(input_count)
        if at not in large
    ]
    state_copies = [
        pltpu.make_async_copy(inputs[-1].at[rows(at)], buffers[-1].at[rows(at)], state_sem.at[at])
        for at in range(blocks)
    ]
    head_copies = [
        pltpu.make_async_copy(inputs[1].at[at], buffers[1].at[at], heads_sem.at[at])
        for at in range(heads)
    ]
    out_copy = pltpu.make_async_copy(inputs[12], buffers[12], out_sem)
    for copy in small_copies:
        copy.start()
    ordered = state_copies + head_copies + [out_copy]
    for copy in ordered[:first_flight]:
        copy.start()
    for copy in small_copies:
        copy.wait()
    for copy in ordered[first_flight:in_flight]:
        copy.start()

    def arrive(at):
        ordered[at].wait()
        if at + in_flight < len(ordered):
            ordered[at + in_flight].start()

    layer_math(
        shares,
        *buffers,
        lambda head: arrive(blocks + head),
        lambda: arrive(blocks + heads),
        arrive,
        *outputs,
        old_part,
        gated_buf,
    )


def stage_body(live, place, *refs):
    inputs = refs[:input_count]
    outputs = refs[input_count : 2 * input_count]
    sems = refs[2 * input_count]

    @pl.when(live[0] == 1)
    def _():
        copies = [
            pltpu.make_async_copy(inputs[at], outputs[at], sems.at[at])
            for at in range(input_count)
        ]
        for copy in copies:
            copy.start()
        for copy in copies:
            copy.wait()


def layer_body(live, place, *refs):
    shares, old_part, gated_buf = refs[-3:]
    parts = shares.shape[0]
    arrived = refs[:parts]
    inputs = refs[parts : parts + input_count]
    older = refs[parts + input_count : parts + input_count + 5]
    sent = refs[parts + input_count + 5]
    newer = refs[parts + input_count + 6 : -3]

    @pl.when(live[0] == 1)
    def _():
        for step in range(parts):
            shares[lax.rem(place[0] + parts - step, parts)] = arrived[step][...]
        def ready(*_):
            return None

        layer_math(shares, *inputs, ready, ready, ready, sent, *newer, old_part, gated_buf)

    @pl.when(live[0] == 0)
    def _():
        for source, target in zip(older, newer):
            target[...] = source[...]


def update_body(old, stepped, decay, b_input, out, state, fresh_buf, in_sems, sems):
    streams, inner, size = state.shape
    heads = decay.shape[1]
    head_size = inner // heads
    blocks = streams // row_block
    chunk_cols = wide_lanes if inner % wide_lanes == 0 else head_size

    def enter(block):
        rows = pl.ds(block * row_block, row_block)
        return pltpu.make_async_copy(old.at[rows], state.at[rows], in_sems.at[block])

    def leave(block):
        rows = pl.ds(block * row_block, row_block)
        return pltpu.make_async_copy(fresh_buf.at[rows], out.at[rows], sems.at[block])

    def step(block, carry):
        first = pl.multiple_of(block * row_block, row_block)
        enter(block).wait()

        @pl.when(block + in_flight < blocks)
        def _():
            enter(block + in_flight).start()

        stepped_rows = stepped[pl.ds(first, row_block), :]
        faded_rows = decay[pl.ds(first, row_block), :]
        b_rows = b_input[pl.ds(first, row_block), :]
        for row in range(row_block):
            b_row = jnp.broadcast_to(b_rows[row : row + 1], (head_size, size))
            for chunk in range(0, inner, chunk_cols):
                line = stepped_rows[row : row + 1, chunk : chunk + chunk_cols]
                spread = jnp.broadcast_to(line.astype(jnp.bfloat16), (size, chunk_cols))
                columns = jnp.transpose(spread).astype(jnp.float32)
                for at in range(0, chunk_cols, head_size):
                    head = (chunk + at) // head_size
                    span = slice(chunk + at, chunk + at + head_size)
                    faded = jnp.broadcast_to(
                        faded_rows[row : row + 1, head : head + 1], (head_size, size)
                    )
                    fresh = (
                        faded * state[first + row, span].astype(jnp.float32)
                        + columns[at : at + head_size] * b_row
                    )
                    fresh_buf[first + row, span] = fresh.astype(jnp.bfloat16)
        leave(block).start()
        return carry

    for block in range(min(in_flight, blocks)):
        enter(block).start()
    lax.fori_loop(0, blocks, step, 0)
    for block in range(blocks):
        leave(block).wait()


def whole(memory=pltpu.VMEM):
    return pl.BlockSpec(memory_space=memory)


def run_first(*operands):
    shares, gain, w_heads, w_bc, w_dt = operands[:5]
    w_out, conv_x_state, conv_bc_state, state = operands[13:]
    parts, streams, share_cols = shares.shape
    heads, width, lanes = w_heads.shape
    head_size = lanes // 2
    inner = heads * head_size
    both = w_bc.shape[1]
    sent_cols = -(-(share_cols + 2) // wide_lanes) * wide_lanes
    flops = 2 * streams * (width * (heads * lanes + both + inner)) + 2 * state.size
    moved = 2 * (w_heads.size + w_bc.size + w_out.size + state.size)
    return pl.pallas_call(
        first_body,
        in_specs=[whole()] + [whole(pltpu.HBM) for _ in operands[1:]],
        out_specs=tuple(whole() for _ in range(6)),
        out_shape=(
            jax.ShapeDtypeStruct((parts, streams, sent_cols), jnp.bfloat16),
            jax.ShapeDtypeStruct(conv_x_state.shape, jnp.bfloat16),
            jax.ShapeDtypeStruct(conv_bc_state.shape, jnp.bfloat16),
            jax.ShapeDtypeStruct((streams, inner), jnp.float32),
            jax.ShapeDtypeStruct((streams, heads), jnp.float32),
            jax.ShapeDtypeStruct((streams, both // 2), jnp.float32),
        ),
        scratch_shapes=[pltpu.VMEM(operand.shape, operand.dtype) for operand in operands[1:]]
        + [
            pltpu.SemaphoreType.DMA((input_count,)),
            pltpu.SemaphoreType.DMA((heads,)),
            pltpu.SemaphoreType.DMA(()),
            pltpu.SemaphoreType.DMA((streams // row_block,)),
            pltpu.VMEM((streams, inner), jnp.float32),
            pltpu.VMEM((streams, inner), jnp.float32),
        ],
        compiler_params=pltpu.CompilerParams(vmem_limit_bytes=44 * 1024 * 1024),
        cost_estimate=pl.CostEstimate(flops=flops, transcendentals=0, bytes_accessed=moved),
        name="first_layer",
    )(*operands)


def run_stage(live, place, *operands):
    moved = sum(operand.size * operand.dtype.itemsize for operand in operands)
    return pl.pallas_call(
        stage_body,
        in_specs=[whole(pltpu.SMEM)] * 2 + [whole(pltpu.HBM) for _ in operands],
        out_specs=tuple(whole() for _ in operands),
        out_shape=tuple(pltpu.VMEM(operand.shape, operand.dtype) for operand in operands),
        scratch_shapes=[pltpu.SemaphoreType.DMA((input_count,))],
        compiler_params=pltpu.CompilerParams(vmem_limit_bytes=1024 * 1024),
        cost_estimate=pl.CostEstimate(flops=40 * moved, transcendentals=0, bytes_accessed=moved),
        name="stage",
    )(live, place, *operands)


def run_layer(live, place, arrived, staged, older):
    parts = len(arrived)
    streams, share_cols = arrived[0].shape
    sent_cols = -(-(share_cols + 2) // wide_lanes) * wide_lanes
    inner = older[2].shape[1]
    outs = (jax.ShapeDtypeStruct((parts, streams, sent_cols), jnp.bfloat16),) + tuple(
        jax.ShapeDtypeStruct(value.shape, value.dtype) for value in older
    )
    moved = sum(operand.size for operand in staged)
    return pl.pallas_call(
        layer_body,
        in_specs=[whole(pltpu.SMEM)] * 2 + [whole() for _ in range(parts + len(staged) + len(older))],
        out_specs=tuple(whole() for _ in outs),
        out_shape=outs,
        scratch_shapes=[
            pltpu.VMEM((parts, streams, share_cols), arrived[0].dtype),
            pltpu.VMEM((streams, inner), jnp.float32),
            pltpu.VMEM((streams, inner), jnp.float32),
        ],
        compiler_params=pltpu.CompilerParams(vmem_limit_bytes=10 * 1024 * 1024),
        cost_estimate=pl.CostEstimate(
            flops=2 * streams * moved, transcendentals=0, bytes_accessed=2 * moved
        ),
        name="layer",
    )(live, place, *arrived, *staged, *older)


def run_update(state, stepped, decay, b_input):
    blocks = state.shape[0] // row_block
    return pl.pallas_call(
        update_body,
        in_specs=[whole(pltpu.HBM)] + [whole() for _ in range(3)],
        out_specs=whole(pltpu.HBM),
        out_shape=jax.ShapeDtypeStruct(state.shape, state.dtype),
        scratch_shapes=[
            pltpu.VMEM(state.shape, state.dtype),
            pltpu.VMEM(state.shape, state.dtype),
            pltpu.SemaphoreType.DMA((blocks,)),
            pltpu.SemaphoreType.DMA((blocks,)),
        ],
        compiler_params=pltpu.CompilerParams(vmem_limit_bytes=24 * 1024 * 1024),
        cost_estimate=pl.CostEstimate(
            flops=40 * state.size, transcendentals=0, bytes_accessed=4 * state.size
        ),
        name="update",
    )(state, stepped, decay, b_input)


def gather_shares(share):
    count = lax.axis_size("tensor")
    spread = jnp.broadcast_to(share[None], (count,) + share.shape)
    return lax.all_to_all(spread, "tensor", 0, 0, tiled=True)


def hand_over(share, source, target, parts, sections):
    def pairs(step):
        moves = [(source, target)]
        if step >= parts - ring_steps:
            moves = [(at, (at + 1) % sections) for at in range(sections)]
        return [
            (start * parts + at, end * parts + (at + step) % parts)
            for start, end in moves
            for at in range(parts)
        ]

    return [lax.ppermute(share, ("section", "tensor"), pairs(step)) for step in range(parts)]


def shards(
    hidden_in,
    pre_gain,
    w_zx,
    w_bc,
    w_dt,
    dt_bias,
    a_log,
    d_skip,
    conv_x_weight,
    conv_x_bias,
    conv_bc_weight,
    conv_bc_bias,
    inner_gain,
    w_out,
    conv_x_state,
    conv_bc_state,
    ssm_state,
):
    section_count = lax.axis_size("section")
    tensor_count = lax.axis_size("tensor")
    section_at = lax.axis_index("section")
    streams, share_cols = hidden_in.shape
    width = w_zx.shape[1]
    heads = w_zx.shape[2]
    head_size = w_zx.shape[3] // 2
    both = w_bc.shape[2]
    inner = heads * head_size
    all_channels = inner * tensor_count
    state = ssm_state[0].reshape(streams, inner, both // 2)
    x_old = jnp.transpose(conv_x_state[0], (1, 2, 0, 3))
    bc_old = jnp.transpose(conv_bc_state[0], (1, 0, 2))
    layer_args = (
        pre_gain,
        jnp.transpose(w_zx[0], (1, 0, 2)),
        w_bc[0],
        jnp.transpose(w_dt[0]),
        dt_bias,
        a_log,
        d_skip,
        jnp.transpose(conv_x_weight[0], (1, 0, 2)),
        jnp.transpose(conv_x_bias, (1, 0, 2)),
        conv_bc_weight[0],
        conv_bc_bias,
        jnp.transpose(inner_gain, (1, 0, 2)),
        w_out[0].reshape(inner, width),
        x_old,
        bc_old,
        state,
    )

    def reduced(sent, share, factors, last):
        got = lax.all_to_all(sent, "tensor", 0, 0, tiled=True)
        if last:
            factors = run_update(state, *factors)
        total = jnp.sum(got.astype(jnp.float32), axis=0)
        squares = total[:, share_cols : share_cols + 1] + total[:, share_cols + 1 : share_cols + 2]
        factor = lax.rsqrt(squares / all_channels + epsilon)
        fresh = (share.astype(jnp.float32) + total[:, :share_cols] * factor).astype(jnp.bfloat16)
        return fresh, factors

    older = (
        x_old,
        bc_old,
        jnp.zeros((streams, inner), jnp.float32),
        jnp.zeros((streams, heads), jnp.float32),
        jnp.zeros((streams, both // 2), jnp.float32),
    )
    def first_live(share, older):
        sent, *newer = run_first(gather_shares(share), *layer_args)
        return reduced(sent, share, (), False)[0], tuple(newer)

    section_share, older = lax.cond(
        section_at == 0, first_live, lambda share, older: (share, older), hidden_in, older
    )
    tensor_at = lax.axis_index("tensor").astype(jnp.int32)
    for tick in range(1, section_count):
        last = tick + 1 == section_count
        section_share, here, place = lax.optimization_barrier(
            (section_share, section_at, tensor_at)
        )
        is_live = here == tick
        live = is_live.astype(jnp.int32)[None]
        place = place[None]
        arrived = hand_over(section_share, tick - 1, tick, tensor_count, section_count)
        staged = run_stage(live, place, *layer_args)
        sent, *older = run_layer(live, place, arrived, staged, older)
        factors = tuple(older[2:]) if last else ()

        def rest(sent, own, kept, factors, last=last):
            return kept, run_update(state, *factors) if last else factors

        section_share, state_new = lax.cond(
            is_live,
            lambda sent, own, kept, factors, last=last: reduced(sent, own, factors, last),
            rest,
            sent,
            arrived[0],
            section_share,
            factors,
        )
    x_new, bc_new = older[:2]
    return (
        section_share[None],
        jnp.transpose(x_new, (2, 0, 1, 3))[None],
        jnp.transpose(bc_new, (1, 0, 2))[None],
        state_new.reshape(ssm_state.shape),
    )


def solution(mesh):
    placed = (
        P(None, "tensor"),
        P("section", None),
        P("section", None, "tensor", None),
        P("section", None, None),
        P("section", None, "tensor"),
        P("section", "tensor"),
        P("section", "tensor"),
        P("section", "tensor"),
        P("section", None, "tensor", None),
        P("section", "tensor", None),
        P("section", None, None),
        P("section", None),
        P("section", "tensor", None),
        P("section", "tensor", None, None),
        P("section", None, None, "tensor", None),
        P("section", None, None, None),
        P("section", None, "tensor", None, None),
    )
    return jax.shard_map(
        shards,
        mesh=mesh,
        in_specs=placed,
        out_specs=(
            P("section", None, "tensor"),
            P("section", None, None, "tensor", None),
            P("section", None, None, None),
            P("section", None, "tensor", None, None),
        ),
        check_vma=False,
    )
```
